512 devices in a mesh: seq: 128 (over y, z, core), head: 4 (over x).
Axes of the slice: x: 4, y: 8, z: 8, core: 2. Of those that a mesh axis runs over, the one named last changes fastest.
Arguments:
- queries: bfloat16 [16384, 1536], P('seq', 'head'), may hold values from -400 to 400
- latent: bfloat16 [16384, 320], P(('seq', 'head')), may hold values from -6 to 6
- w_kv_up: bfloat16 [256, 2048], P(None, 'head'), may hold values from -0.375 to 0.375
Outputs:
- attended: bfloat16 [16384, 1024], P('seq', 'head')
The draws below stay inside these ranges and needn't reach their ends.
All inputs are finite; a program needn't handle non-finite values.
Results may differ from the reference program's by a relative error of at most 0.004.
Values may be sent and summed in bfloat16 or wider, within the bound.
A program may use at most 64 MiB of HBM per device.

```python
import jax
import jax.numpy as jnp
from jax import lax

D_LATENT = 256
ROPE = 64
NOPE = 128
VDIM = 128
HEADS = 8
TOK_DEV = 128
SEQS = 1
LENGTH = 16384
TOKENS = 16384


def latent_field(key):
    sample = jax.random.normal(jax.random.fold_in(key, 11), (TOKENS, D_LATENT + ROPE), jnp.float32)
    return jnp.clip(sample, -6.0, 6.0)


def draw_latent(key, part):
    return latent_field(key).astype(jnp.bfloat16)


def draw_queries(key, part):
    sample = jax.random.normal(jax.random.fold_in(key, 23), (TOKENS, HEADS, NOPE + ROPE), jnp.float32)
    sample = 2.0 * jnp.clip(sample, -4.0, 4.0)
    return sample.reshape(TOKENS, HEADS * (NOPE + ROPE)).astype(jnp.bfloat16)


def shard_levels(stream_key, extent, cuts, smallest, top_value):
    def one(axis_at, parts):
        heights = jax.random.uniform(jax.random.fold_in(jax.random.fold_in(stream_key, 6), axis_at), (parts,), jnp.float32, smallest / len(cuts), top_value / len(cuts))
        return jnp.repeat(jnp.exp(heights), extent[axis_at] // parts).reshape((-1,) + (1,) * (len(extent) - axis_at - 1))

    loudness = one(*cuts[0])
    for cut in cuts[1:]:
        loudness = loudness * one(*cut)
    return loudness


def scatter_about(own_key, dims, deviation, most, cuts=(), kind=jnp.bfloat16):
    array = jax.random.normal(own_key, dims, jnp.float32) * deviation
    if len(cuts) > 0:
        array = shard_levels(own_key, dims, cuts, -0.22, 0.18) * array
    return jnp.clip(array, min=-most, max=most).astype(kind)


def setup_inputs(seed: int = 0) -> dict:
    keys = jax.random.split(jax.random.key(seed), 4)
    queries = draw_queries(jax.random.fold_in(keys[3], 71), 0)
    latent = draw_latent(jax.random.fold_in(keys[3], 71), 0)
    w_kv_up = scatter_about(keys[2], (D_LATENT, HEADS * (NOPE + VDIM)), D_LATENT ** -0.5, 0.375, ((1, 4),))
    return dict(queries=queries, latent=latent, w_kv_up=w_kv_up)


MASKED = -1e30


def reference(queries, latent, w_kv_up):
    head_width = NOPE + VDIM
    score_scale = (NOPE + ROPE) ** -0.5
    highest = lax.Precision.HIGHEST

    def one_sequence(seq_index):
        first_row = seq_index * LENGTH
        seq_latent = lax.dynamic_slice_in_dim(latent, first_row, LENGTH, 0)
        seq_queries = lax.dynamic_slice_in_dim(queries, first_row, LENGTH, 0)
        key_value = jnp.dot(seq_latent[:, :D_LATENT], w_kv_up, preferred_element_type=jnp.float32)
        key_value = key_value.reshape(LENGTH, HEADS, head_width)
        key_nope = key_value[:, :, :NOPE]
        values = key_value[:, :, NOPE:]
        key_rope = seq_latent[:, D_LATENT:].astype(jnp.float32)
        query_all = seq_queries.reshape(LENGTH, HEADS, NOPE + ROPE).astype(jnp.float32)
        blocks_out = []
        for block_index in range(LENGTH // TOK_DEV):
            low_row = block_index * TOK_DEV
            high_row = low_row + TOK_DEV
            query_block = query_all[low_row:high_row]
            scores = jnp.einsum('qhd,khd->hqk', query_block[:, :, :NOPE], key_nope[:high_row], precision=highest)
            scores = scores + jnp.einsum('qhd,kd->hqk', query_block[:, :, NOPE:], key_rope[:high_row], precision=highest)
            scores = scores * score_scale
            allowed = jnp.arange(high_row)[None, :] <= (low_row + jnp.arange(TOK_DEV))[:, None]
            scores = jnp.where(allowed[None], scores, MASKED)
            row_max = jnp.max(scores, axis=2, keepdims=True)
            weights = jnp.where(allowed[None], jnp.exp(scores - row_max), 0.0)
            totals = jnp.sum(weights, axis=2)
            rounded = lax.optimization_barrier(weights.astype(jnp.bfloat16)).astype(jnp.float32)
            summed = jnp.einsum('hqk,khd->hqd', rounded, values[:high_row], precision=highest)
            result = summed / totals[:, :, None]
            blocks_out.append(jnp.transpose(result, (1, 0, 2)).reshape(TOK_DEV, HEADS * VDIM))
        return jnp.concatenate(blocks_out, axis=0).astype(jnp.bfloat16)

    pieces = lax.map(one_sequence, jnp.arange(SEQS, dtype=jnp.int32))
    return pieces.reshape(TOKENS, HEADS * VDIM)
```

```python
import math

import jax
import jax.numpy as jnp
from jax import lax
from jax.experimental import pallas as pl
from jax.experimental.pallas import tpu as pltpu
from jax.sharding import PartitionSpec as P

D_LATENT = 256
ROPE = 64
NOPE = 128
VDIM = 128
QW = NOPE + ROPE
MASKED = -1e30
FLOOR = -1e29
SCALE = QW ** (-0.5) * math.log2(math.e)
F32 = jnp.float32
BF16 = jnp.bfloat16


def two_pieces(value):
    high = value.astype(BF16)
    low = (value - high.astype(F32)).astype(BF16)
    return high, low


def prepare_pair(q_all, w_all, side_ref, row):
    for j in range(2):
        q = q_all[:, j * QW : (j + 1) * QW]
        nope = q[:, :NOPE].astype(BF16)
        rope = q[:, NOPE:] * SCALE
        w_key = w_all[:, j * 256 : j * 256 + 128]
        side = lax.dot_general(nope, w_key, (((1,), (1,)), ((), ())), preferred_element_type=F32)
        high, low = two_pieces(side * SCALE)
        rows = pl.ds(row + j * 128, 128)
        side_ref[rows, 0:256] = high
        side_ref[rows, 256:512] = low
        rope_high, rope_low = two_pieces(rope)
        side_ref[rows, 512:640] = jnp.concatenate([rope_high, rope_low], axis=1)


def flash_rows(side_ref, key, key_t, allowed, m_ref, l_ref, acc_ref, row, count):
    rows = pl.ds(row, count)
    scores = jnp.dot(side_ref[rows, :], key_t, preferred_element_type=F32)
    if allowed is not None:
        scores = jnp.where(allowed, scores, MASKED)
    old_max = m_ref[rows, :]
    new_max = jnp.maximum(old_max, jnp.max(scores, axis=1, keepdims=True))
    factor = jnp.exp2(old_max - new_max)
    weights = jnp.exp2(scores - new_max[:, :1])
    lanes = weights[:, 0:128]
    for piece in range(1, weights.shape[1] // 128):
        lanes = lanes + weights[:, piece * 128 : (piece + 1) * 128]
    l_ref[rows, :] = l_ref[rows, :] * factor + lanes
    update = jnp.dot(weights.astype(BF16), key, preferred_element_type=F32)
    acc_ref[rows, :] = acc_ref[rows, :] * jnp.concatenate([factor, factor], axis=1) + update
    m_ref[rows, :] = new_max


def finish_head(w_all, m_ref, l_ref, acc_ref, row, j):
    rows = pl.ds(row + j * 128, 128)
    total = jnp.sum(l_ref[rows, :], axis=1, keepdims=True)
    normal = acc_ref[rows, :] / jnp.maximum(total, 1.0)
    high, low = two_pieces(normal)
    w_value = w_all[:, j * 256 + 128 : j * 256 + 256]
    out = jnp.dot(high, w_value, preferred_element_type=F32)
    out = out + jnp.dot(low, w_value, preferred_element_type=F32)
    m_row = m_ref[rows, :].T[0:1, :]
    l_row = jnp.broadcast_to(total, (128, 128)).T[0:1, :]
    return out, m_row, l_row


CHUNK = 256


def kernel(q_ref, w_ref, k_ref, o_ref, st_ref, side_ref, m_ref, l_ref, acc_ref, kt_ref):
    group = lax.axis_index("seq")
    part = lax.axis_index("head")
    m_ref[...] = jnp.full_like(m_ref, FLOOR)
    l_ref[...] = jnp.zeros_like(l_ref)
    acc_ref[...] = jnp.zeros_like(acc_ref)
    for p in range(4):
        prepare_pair(q_ref[p].astype(F32), w_ref[p], side_ref, p * 256)

    def one_chunk(c, carry):
        key = k_ref[pl.ds(c * CHUNK, CHUNK), 0:256]
        rope = k_ref[pl.ds(c * CHUNK, CHUNK), 256:320]
        key_t = key.T
        rope_t = rope.T
        kt_ref[0:256, :] = key_t
        kt_ref[256:512, :] = key_t
        kt_ref[512:576, :] = rope_t
        kt_ref[576:640, :] = rope_t
        col = lax.broadcasted_iota(jnp.int32, (1, CHUNK), 1)
        key_pos = (c * (CHUNK // 32) + col // 32) * 128 + part * 32 + col % 32
        query_pos = group * 128 + lax.broadcasted_iota(jnp.int32, (128, 1), 0)
        allowed = key_pos <= query_pos
        allowed = jnp.concatenate([allowed, allowed], axis=0)
        for p in range(4):
            flash_rows(side_ref, key, kt_ref[...], allowed, m_ref, l_ref, acc_ref, p * 256, 256)
        return carry

    lax.fori_loop(0, group * 32 // CHUNK + 1, one_chunk, 0)
    for p in range(4):
        st_ref[p] = jnp.zeros((8, 128), F32)
        for j in range(2):
            out, m_row, l_row = finish_head(w_ref[p], m_ref, l_ref, acc_ref, p * 256, j)
            o_ref[p, :, j * 128 : (j + 1) * 128] = out
            st_ref[p, 2 * j : 2 * j + 1, :] = m_row
            st_ref[p, 2 * j + 1 : 2 * j + 2, :] = l_row


def body(queries, latent, w_kv_up):
    keys = lax.all_gather(latent, "seq", axis=0, tiled=True)
    q_all = lax.all_gather(queries, "head", axis=0)
    w_all = lax.all_gather(w_kv_up, "head", axis=0)
    out, stats = pl.pallas_call(
        kernel,
        out_shape=[
            jax.ShapeDtypeStruct((4, 128, 256), F32),
            jax.ShapeDtypeStruct((4, 8, 128), F32),
        ],
        in_specs=[pl.BlockSpec(memory_space=pltpu.VMEM)] * 3,
        out_specs=[pl.BlockSpec(memory_space=pltpu.VMEM)] * 2,
        scratch_shapes=[
            pltpu.VMEM((1024, 640), BF16),
            pltpu.VMEM((1024, 128), F32),
            pltpu.VMEM((1024, 128), F32),
            pltpu.VMEM((1024, 256), F32),
            pltpu.VMEM((640, CHUNK), BF16),
        ],
        compiler_params=pltpu.CompilerParams(vmem_limit_bytes=40 * 1024 * 1024),
    )(q_all, w_all, keys)
    out = lax.all_to_all(out, "head", 0, 0, tiled=True)
    stats = lax.all_to_all(stats, "head", 0, 0, tiled=True)
    heads = []
    for j in range(2):
        m = stats[:, 2 * j]
        total = stats[:, 2 * j + 1]
        weight = jnp.exp2(m - jnp.max(m, axis=0, keepdims=True)) * total
        weight = weight / jnp.sum(weight, axis=0, keepdims=True)
        heads.append(jnp.sum(out[:, :, j * 128 : (j + 1) * 128] * weight[:, :, None], axis=0))
    return jnp.concatenate(heads, axis=1).astype(BF16)


def solution(mesh):
    in_specs = (P("seq", "head"), P(("seq", "head"), None), P(None, "head"))
    out_specs = P("seq", "head")
    return jax.shard_map(body, mesh=mesh, in_specs=in_specs, out_specs=out_specs, check_vma=False)
```

```python
import math

import jax
import jax.numpy as jnp
from jax import lax
from jax.experimental import pallas as pl
from jax.experimental.pallas import tpu as pltpu
from jax.sharding import PartitionSpec as P

D_LATENT = 256
ROPE = 64
NOPE = 128
VDIM = 128
QW = NOPE + ROPE
MASKED = -1e30
FLOOR = -1e29
SCALE = QW ** (-0.5) * math.log2(math.e)
F32 = jnp.float32
BF16 = jnp.bfloat16
MESH = pl.DeviceIdType.MESH
CH = 256
OFFSETS = (0, 1, 7, 2, 6, 3, 5, 4)


def two_pieces(value):
    high = value.astype(BF16)
    low = (value - high.astype(F32)).astype(BF16)
    return high, low


def prepare_pair(q_ref, w_ref, side_ref, p):
    q = q_ref[p].astype(F32)
    rope = (q[:, 128:256].T[0:64], q[:, 256:384].T[64:128])
    for j in range(2):
        nope = q[:, j * QW : j * QW + NOPE].astype(BF16)
        side = lax.dot_general(
            w_ref[p, 2 * j], nope, (((1,), (1,)), ((), ())), preferred_element_type=F32
        )
        high, low = two_pieces(side * SCALE)
        rope_high, rope_low = two_pieces(rope[j] * SCALE)
        columns = slice(j * 128, (j + 1) * 128)
        side_ref[p, 0:256, columns] = high
        side_ref[p, 256:512, columns] = low
        side_ref[p, 512:640, columns] = jnp.concatenate([rope_high, rope_low], axis=0)


def load_chunk(k_ref, c, lhs_ref, kt_ref):
    key = k_ref[c, :, 0:256]
    rope = k_ref[c, :, 256:320]
    lhs_ref[:, 0:256] = key
    lhs_ref[:, 256:384] = jnp.concatenate([rope, rope], axis=1)
    kt_ref[...] = key.T


def scores_of(lhs_ref, side_ref, s_ref, p):
    key = lhs_ref[:, 0:256]
    lhs = jnp.concatenate([key, key, lhs_ref[:, 256:384]], axis=1)
    s_ref[p] = jnp.dot(lhs, side_ref[p], preferred_element_type=F32)


def soften(s_ref, kt_ref, bias_ref, st_ref, acc_ref, p):
    bias = bias_ref[...]
    scores = s_ref[p] + jnp.concatenate([bias, bias], axis=1)
    old = st_ref[p, 0:1, :]
    new = jnp.maximum(old, jnp.max(scores, axis=0, keepdims=True))
    factor = jnp.exp2(old - new)
    weights = jnp.exp2(scores - new)
    st_ref[p, 1:2, :] = st_ref[p, 1:2, :] * factor + jnp.sum(weights, axis=0, keepdims=True)
    update = jnp.dot(kt_ref[...], weights.astype(BF16), preferred_element_type=F32)
    acc_ref[p] = acc_ref[p] * factor + update
    st_ref[p, 0:1, :] = new


def finish_pair(w_ref, st_ref, acc_ref, p):
    outs = []
    for j in range(2):
        columns = slice(j * 128, (j + 1) * 128)
        total = jnp.maximum(st_ref[p, 1:2, columns], 1.0)
        high, low = two_pieces(acc_ref[p, :, columns] / total)
        value_t = w_ref[p, 2 * j + 1].T
        out = jnp.dot(value_t, high, preferred_element_type=F32)
        outs.append(out + jnp.dot(value_t, low, preferred_element_type=F32))
    return outs


def kernel(
    q_hbm, lat_hbm, w_hbm, o_ref,
    k_ref, q_ref, w_ref, side_ref, acc_ref, st_ref, base_ref,
    lhs_a, kt_a, s_a, bias_a, lhs_b, kt_b, s_b, bias_b,
    out_ref, gout_ref, gst_ref,
    load_sem, near_send, near_recv, k_recv, ring_send, sib_send,
    x_send, x_recv, w_recv, wsib_send, out_send, out_recv, st_send, st_recv,
):
    seq = lax.axis_index("seq")
    x = lax.axis_index("head")
    core = lax.rem(seq, 2)
    z = lax.rem(lax.div(seq, 2), 8)
    y = lax.div(seq, 16)
    ia = z + core * (y - z)
    ib = y + core * (z - y)

    def at(a, b):
        a = lax.rem(a, 8)
        b = lax.rem(b, 8)
        to_y = b + core * (a - b)
        to_z = a + core * (b - a)
        return ((to_y * 8 + to_z) * 2 + core, x)

    sibling = (seq + 1 - 2 * core, x)
    up = at(ia, ib + 1)
    down = at(ia, ib + 7)

    def peer(e):
        return (seq, lax.rem(x + e, 4))

    def copy(src, dst, send, recv, to):
        return pltpu.make_async_remote_copy(
            src_ref=src, dst_ref=dst, send_sem=send, recv_sem=recv, device_id=to, device_id_type=MESH
        )

    loads = [
        pltpu.make_async_copy(lat_hbm, k_ref.at[0, pl.ds(0, 32)], load_sem.at[0]),
        pltpu.make_async_copy(q_hbm, q_ref.at[0], load_sem.at[1]),
    ]
    for part in range(4):
        loads.append(
            pltpu.make_async_copy(
                w_hbm.at[:, pl.ds(part * 128, 128)], w_ref.at[0, part], load_sem.at[2 + part]
            )
        )
    for load in loads:
        load.start()

    barrier = pltpu.get_barrier_semaphore()
    for e in range(1, 8):
        pl.semaphore_signal(barrier, inc=1, device_id=at(ia + e, ib), device_id_type=MESH)
    for to in (up, down, sibling, peer(1), peer(2), peer(3)):
        pl.semaphore_signal(barrier, inc=1, device_id=to, device_id_type=MESH)

    row = lax.broadcasted_iota(jnp.int32, (CH, 128), 0)
    slot = row // 32
    half = (slot + 1) // 2
    offset = jnp.where(slot % 2 == 1, half, (8 - half) % 8)
    for which in range(2):
        color = core if which == 0 else 1 - core
        start = z + color * (y - z)
        along = (start + offset) % 8
        base_ref[which] = along * (256 + color * 1792) + color * 128 + x * 32 + row % 32

    def set_bias(bias_ref, c):
        hop = lax.div(c + 2, 4)
        late = lax.rem(c + 2, 4)
        edge = jnp.logical_or(c < 2, c > 13)
        which = jnp.where(edge, lax.rem(c, 2), lax.div(late, 2))
        db = jnp.where(c < 2, 0, jnp.where(c > 13, 4, jnp.where(lax.rem(c, 2) == 0, 8 - hop, hop)))
        color = core + which * (1 - 2 * core)
        start = y + color * (z - y)
        moved = lax.rem(start + db, 8) * (2048 - color * 1792)
        query = seq * 128 + lax.broadcasted_iota(jnp.int32, (CH, 128), 1)
        bias_ref[...] = jnp.where(base_ref[which] <= query - moved, 0.0, MASKED)

    for load in loads:
        load.wait()
    pl.semaphore_wait(barrier, 13)

    near = []
    for j in range(1, 8):
        e = (8 - OFFSETS[j]) % 8
        near.append(
            copy(
                k_ref.at[0, pl.ds(0, 32)], k_ref.at[0, pl.ds(j * 32, 32)],
                near_send.at[j], near_recv.at[j], at(ia + e, ib),
            )
        )
    for one in near:
        one.start()
    w_key = []
    w_value = []
    q_copies = []
    for e in (1, 3, 2):
        s = 4 - e
        w_key.append(
            copy(w_ref.at[0, 2 * core], w_ref.at[s, 2 * core], x_send.at[0, e], x_recv.at[0, s], peer(e))
        )
        q_copies.append(copy(q_ref.at[0], q_ref.at[s], x_send.at[1, e], x_recv.at[1, s], peer(e)))
        w_value.append(
            copy(
                w_ref.at[0, 2 * core + 1], w_ref.at[s, 2 * core + 1],
                x_send.at[2, e], x_recv.at[2, s], peer(e),
            )
        )
    for one in w_key + q_copies + w_value:
        one.start()

    st_ref[:, 0:1, :] = jnp.full((4, 1, 256), FLOOR, F32)
    st_ref[:, 1:8, :] = jnp.zeros((4, 7, 256), F32)
    acc_ref[...] = jnp.zeros_like(acc_ref)
    prepare_pair(q_ref, w_ref, side_ref, 0)

    def quarter(c, q):
        return k_ref.at[c, pl.ds(q * 64, 64)]

    def ring(direction, hop, src, dst, q, to):
        return copy(quarter(src, q), quarter(dst, q), ring_send.at[direction, hop, q], k_recv.at[dst, q], to)

    def across(src, dst, q):
        return copy(quarter(src, q), quarter(dst, q), sib_send.at[dst, q], k_recv.at[dst, q], sibling)

    def arrived(c, q):
        copy(quarter(c, q), quarter(c, q), sib_send.at[c, q], k_recv.at[c, q], sibling).wait_recv()

    for q in range(4):
        for j in (2 * q, 2 * q + 1):
            if j > 0:
                near[j - 1].wait_recv()
        ring(0, 0, 0, 2, q, up).start()
        ring(1, 0, 0, 3, q, down).start()
        across(0, 1, q).start()

    def w_across(s, part):
        return copy(
            w_ref.at[s, 2 * core + part], w_ref.at[s, 2 * core + part],
            wsib_send.at[part, s], w_recv.at[part, s], sibling,
        )

    def w_arrived(s, part):
        other = 2 - 2 * core + part
        copy(
            w_ref.at[s, other], w_ref.at[s, other], wsib_send.at[part, s], w_recv.at[part, s], sibling
        ).wait_recv()

    for s in (3, 1, 2):
        copy(w_ref.at[0, 2 * core], w_ref.at[s, 2 * core], x_send.at[0, s], x_recv.at[0, s], peer(s)).wait_recv()
        w_across(s, 0).start()

    for q in range(4):
        arrived(2, q)
        ring(0, 1, 2, 6, q, up).start()
        across(2, 4, q).start()
        arrived(3, q)
        ring(1, 1, 3, 7, q, down).start()
        across(3, 5, q).start()

    for s in (3, 1, 2):
        copy(q_ref.at[0], q_ref.at[s], x_send.at[1, s], x_recv.at[1, s], peer(s)).wait_recv()
        w_arrived(s, 0)
        prepare_pair(q_ref, w_ref, side_ref, s)

    def event(i, part):
        q = 2 * lax.rem(i, 2) + part

        @pl.when(i < 4)
        def _():
            hop = 2 + lax.div(i, 2)
            above = 4 * hop - 2
            below = 4 * hop - 1
            arrived(above, q)

            @pl.when(jnp.logical_or(i < 2, q < 2))
            def _():
                ring(0, hop, above, above + 4, q, up).start()

            across(above, above + 2, q).start()
            arrived(below, q)

            @pl.when(i < 2)
            def _():
                ring(1, hop, below, below + 4, q, down).start()

            @pl.when(i == 3)
            def _():
                ring(1, hop, below, below + 3, q, down).start()

            across(below, below + 2, q).start()

        @pl.when(jnp.logical_and(i >= 4, i < 6))
        def _():
            arrived(14, q)
            across(14, 15, q).start()

    def bundle_arrived(c):
        for q in range(4):
            arrived(c, q)

    first = (lhs_a, kt_a, s_a, bias_a)
    second = (lhs_b, kt_b, s_b, bias_b)

    load_chunk(k_ref, 0, lhs_a, kt_a)
    set_bias(bias_a, 0)
    for p in range(4):
        scores_of(lhs_a, side_ref, s_a, p)

    def half_step(c, now, later):
        load_chunk(k_ref, c + 1, later[0], later[1])
        set_bias(later[3], c + 1)
        for p in range(4):
            scores_of(later[0], side_ref, later[2], p)
            soften(now[2], now[1], now[3], st_ref, acc_ref, p)

    def two_chunks(i, carry):
        event(i, 0)

        @pl.when(jnp.logical_or(lax.rem(i, 2) == 0, i == 7))
        def _():
            bundle_arrived(2 * i + 1)

        half_step(2 * i, first, second)
        event(i, 1)

        @pl.when(jnp.logical_and(lax.rem(i, 2) == 1, i < 7))
        def _():
            bundle_arrived(2 * i + 2)

        @pl.when(i < 7)
        def _():
            half_step(2 * i + 1, second, first)

        return carry

    lax.fori_loop(0, 8, two_chunks, 0)
    for p in range(4):
        soften(s_b, kt_b, bias_b, st_ref, acc_ref, p)

    for s in (3, 1, 2):
        copy(
            w_ref.at[0, 2 * core + 1], w_ref.at[s, 2 * core + 1], x_send.at[2, s], x_recv.at[2, s], peer(s)
        ).wait_recv()
        w_across(s, 1).start()

    def send_out(e):
        s = 4 - e
        copy(st_ref.at[e], gst_ref.at[s], st_send.at[e], st_recv.at[s], peer(e)).start()
        copy(out_ref.at[e], gout_ref.at[s], out_send.at[e], out_recv.at[s], peer(e)).start()

    order = (2, 1, 3)
    for n, e in enumerate(order):
        w_arrived(e, 1)
        out = finish_pair(w_ref, st_ref, acc_ref, e)
        out_ref[e, 0:128, :] = out[0].astype(BF16)
        out_ref[e, 128:256, :] = out[1].astype(BF16)
        if n > 0:
            send_out(order[n - 1])
    own = finish_pair(w_ref, st_ref, acc_ref, 0)
    send_out(order[2])

    for s in (2, 3, 1):
        copy(st_ref.at[s], gst_ref.at[s], st_send.at[s], st_recv.at[s], peer(s)).wait_recv()
        copy(out_ref.at[s], gout_ref.at[s], out_send.at[s], out_recv.at[s], peer(s)).wait_recv()
    for j in range(2):
        columns = slice(j * 128, (j + 1) * 128)
        tops = [st_ref[0, 0:1, columns]] + [gst_ref[s, 0:1, columns] for s in (1, 2, 3)]
        sums = [st_ref[0, 1:2, columns]] + [gst_ref[s, 1:2, columns] for s in (1, 2, 3)]
        parts = [own[j]] + [gout_ref[s, columns, :].astype(F32) for s in (1, 2, 3)]
        top = jnp.maximum(jnp.maximum(tops[0], tops[1]), jnp.maximum(tops[2], tops[3]))
        shares = [jnp.exp2(tops[s] - top) * sums[s] for s in range(4)]
        whole = shares[0] + shares[1] + shares[2] + shares[3]
        result = parts[0] * (shares[0] / whole)
        for s in range(1, 4):
            result = result + parts[s] * (shares[s] / whole)
        o_ref[:, columns] = result.T.astype(BF16)

    for one in near + w_key + q_copies + w_value:
        one.wait_send()
    for e in (1, 2, 3):
        copy(st_ref.at[e], gst_ref.at[e], st_send.at[e], st_recv.at[e], peer(e)).wait_send()
        copy(out_ref.at[e], gout_ref.at[e], out_send.at[e], out_recv.at[e], peer(e)).wait_send()
        w_across(e, 0).wait_send()
        w_across(e, 1).wait_send()
    for q in range(4):
        for hop in range(3):
            ring(0, hop, 0, 2, q, up).wait_send()
            ring(1, hop, 0, 2, q, down).wait_send()
        ring(0 if q < 2 else 1, 3, 0, 2, q, up).wait_send()
        for c in (1, 4, 5, 8, 9, 12, 13, 15):
            across(0, c, q).wait_send()


def body(queries, latent, w_kv_up):
    dma = pltpu.SemaphoreType.DMA
    chunk = [
        pltpu.VMEM((CH, 384), BF16),
        pltpu.VMEM((256, CH), BF16),
        pltpu.VMEM((4, CH, 256), F32),
        pltpu.VMEM((CH, 128), F32),
    ]
    return pl.pallas_call(
        kernel,
        out_shape=jax.ShapeDtypeStruct((128, 256), BF16),
        in_specs=[pl.BlockSpec(memory_space=pl.ANY)] * 3,
        out_specs=pl.BlockSpec(memory_space=pltpu.VMEM),
        scratch_shapes=[
            pltpu.VMEM((16, CH, 320), BF16),
            pltpu.VMEM((4, 128, 384), BF16),
            pltpu.VMEM((4, 4, 256, 128), BF16),
            pltpu.VMEM((4, 640, 256), BF16),
            pltpu.VMEM((4, 256, 256), F32),
            pltpu.VMEM((4, 8, 256), F32),
            pltpu.VMEM((2, CH, 128), jnp.int32),
            *chunk,
            *chunk,
            pltpu.VMEM((4, 256, 128), BF16),
            pltpu.VMEM((4, 256, 128), BF16),
            pltpu.VMEM((4, 8, 256), F32),
            dma((6,)),
            dma((8,)),
            dma((8,)),
            dma((16, 4)),
            dma((2, 4, 4)),
            dma((16, 4)),
            dma((3, 4)),
            dma((3, 4)),
            dma((2, 4)),
            dma((2, 4)),
            dma((4,)),
            dma((4,)),
            dma((4,)),
            dma((4,)),
        ],
        compiler_params=pltpu.CompilerParams(
            vmem_limit_bytes=40 * 1024 * 1024, collective_id=0, has_side_effects=True
        ),
    )(queries, latent, w_kv_up)


def solution(mesh):
    in_specs = (P("seq", "head"), P(("seq", "head"), None), P(None, "head"))
    out_specs = P("seq", "head")
    return jax.shard_map(body, mesh=mesh, in_specs=in_specs, out_specs=out_specs, check_vma=False)
```
